32 devices in a mesh: league: 2 (over x), seq: 16 (over z, y, core).
Axes of the slice: x: 2, y: 2, z: 4, core: 2. Of those that a mesh axis runs over, the one named last changes fastest.
Arguments:
- queries: bfloat16 [6144, 1792], P(('league', 'seq')), parts along dimension 0, may hold values from -100 to 100
- key_rows: bfloat16 [6144, 256], P(('league', 'seq')), parts along dimension 0, may hold values from -4 to 4
- value_rows: bfloat16 [6144, 256], P(('league', 'seq')), parts along dimension 0, may hold values from -6 to 6
- residual: bfloat16 [6144, 3584], P(('league', 'seq')), parts along dimension 0, may hold values from -6 to 6
- out_weight: bfloat16 [1792, 3584], P('seq'), may hold values from -0.125 to 0.125
- norm_gain: float32 [3584], replicated, may hold values from 0.1 to 1.9
- value_head: float32 [3584], replicated, may hold values from -0.09375 to 0.09375
- valid_length: int32 [2], P('league'), parts along dimension 0, may hold values from 1537 to 3072
Outputs:
- stream: bfloat16 [6144, 3584], P(('league', 'seq')), parts along dimension 0
- values: float32 [6144], P(('league', 'seq')), parts along dimension 0
The draws below stay inside these ranges and needn't reach their ends.
There are 2 independent parts, one for each index of `league`. The reference program is written for one: setup_inputs(seed, part) draws one part's arguments, and reference() takes and returns one part's arrays. A program takes and returns all parts, laid end to end along the dimension named above; an argument that names none is the same for every part. Nothing has to cross between parts.
All inputs are finite; a program needn't handle non-finite values.
Results may differ from the reference program's by a relative error of at most 0.0085.
Values may be sent and summed in bfloat16 or wider, within the bound.
A program may use at most 128 MiB of HBM per device.

```python
import math
import jax
import jax.numpy as jnp
from jax import lax

D = 3584
HEADS = 14
KV_HEADS = 2
HEAD_DIM = 128
SEQ = 3072


def paired_fields(seed_key):
    folded = jax.random.fold_in(seed_key, 4242)
    key_query, key_keys = jax.random.split(folded, 2)
    width_query = HEADS * HEAD_DIM
    width_keys = KV_HEADS * HEAD_DIM
    query_field = 2.5 * jnp.clip(jax.random.normal(key_query, (SEQ, width_query), jnp.float32), -4.0, 4.0)
    key_field = jnp.clip(jax.random.normal(key_keys, (SEQ, width_keys), jnp.float32), -4.0, 4.0)
    return (query_field, key_field)


def draw_queries(key, part):
    return paired_fields(key)[0].astype(jnp.bfloat16)


def draw_key_rows(key, part):
    return paired_fields(key)[1].astype(jnp.bfloat16)


def block_levels(own_key, shape, cuts, smallest, top_value):
    loudness, own = 1.0, jax.random.fold_in(own_key, 6)
    for position, parts in cuts:
        steps = jnp.exp(jax.random.uniform(jax.random.fold_in(own, position), (parts,), jnp.float32, smallest / len(cuts), top_value / len(cuts)))
        loudness = loudness * jnp.repeat(steps, shape[position] // parts).reshape([-1 if axis == position else 1 for axis in range(len(shape))])
    return loudness


def normal_values(own_key, dims, deviation, limit, shards=(), kind=jnp.bfloat16):
    array = deviation * jax.random.normal(own_key, dims, jnp.float32)
    if shards:
        array = array * block_levels(own_key, dims, shards, -0.22, 0.18)
    return jnp.clip(array, -limit, limit).astype(kind)


def setup_inputs(seed: int = 0, part: int = 0) -> dict:
    key_list = jax.random.split(jax.random.key(seed), 9)
    part_splits = jax.random.split(jax.random.fold_in(key_list[8], part), 9)
    queries = draw_queries(jax.random.fold_in(jax.random.fold_in(key_list[8], part), 71), part)
    key_rows = draw_key_rows(jax.random.fold_in(jax.random.fold_in(key_list[8], part), 71), part)
    value_rows = normal_values(part_splits[2], (SEQ, KV_HEADS * HEAD_DIM), 1.0, 6.0, ((0, 16),))
    residual = normal_values(part_splits[3], (SEQ, D), 1.0, 6.0, ((0, 16),))
    out_weight = normal_values(key_list[4], (HEADS * HEAD_DIM, D), (HEADS * HEAD_DIM) ** -0.5, 0.125, ((0, 16),))
    norm_gain = jnp.clip(1.0 + 0.18 * jax.random.normal(key_list[5], (D,), jnp.float32), 0.1, 1.9)
    value_head = normal_values(key_list[6], (D,), D ** -0.5, 0.09375, (), jnp.float32)
    valid_length = jax.random.randint(part_splits[7], (1,), SEQ // 2 + 1, SEQ + 1).astype(jnp.int32)
    return {"queries": queries, "key_rows": key_rows, "value_rows": value_rows, "residual": residual, "out_weight": out_weight, "norm_gain": norm_gain, "value_head": value_head, "valid_length": valid_length}


def reference(queries, key_rows, value_rows, residual, out_weight, norm_gain, value_head, valid_length):
    seq_rows = queries.shape[0]
    groups = KV_HEADS
    repeats = HEADS // KV_HEADS
    valid_upto = valid_length[0]
    positions = jnp.arange(seq_rows, dtype=jnp.int32)
    query_wide = queries.astype(jnp.float32).reshape(seq_rows, groups, repeats, HEAD_DIM)
    key_wide = key_rows.astype(jnp.float32).reshape(seq_rows, groups, HEAD_DIM)
    value_wide = value_rows.astype(jnp.float32).reshape(seq_rows, groups, HEAD_DIM)
    block_rows = math.gcd(seq_rows, 512)
    score_scale = HEAD_DIM ** (-0.5)

    def one_block(index):
        first_row = (index * block_rows).astype(jnp.int32)
        query_block = lax.dynamic_slice_in_dim(query_wide, first_row, block_rows, 0)
        query_pos = first_row + jnp.arange(block_rows, dtype=jnp.int32)
        scores = jnp.einsum('qgrd,kgd->qgrk', query_block, key_wide) * score_scale
        allowed = positions[None, None, None, :] <= query_pos[:, None, None, None]
        row_max = lax.optimization_barrier(jnp.max(jnp.where(allowed, scores, -jnp.inf), axis=-1))
        weights = jnp.where(allowed, jnp.exp(scores - row_max[..., None]), 0.0)
        totals = lax.optimization_barrier(jnp.sum(weights, axis=-1))
        rounded = lax.optimization_barrier(weights.astype(jnp.bfloat16)).astype(jnp.float32)
        mixed = jnp.einsum('qgrk,kgd->qgrd', rounded, value_wide) / totals[..., None]
        mixed = jnp.where((query_pos < valid_upto)[:, None, None, None], mixed, 0.0)
        return mixed.reshape(block_rows, HEADS * HEAD_DIM).astype(jnp.bfloat16)
    attended = lax.map(one_block, jnp.arange(seq_rows // block_rows, dtype=jnp.int32))
    attended = attended.reshape(seq_rows, HEADS * HEAD_DIM)
    projected = jnp.dot(attended, out_weight, preferred_element_type=jnp.float32)
    stream = (residual.astype(jnp.float32) + projected).astype(jnp.bfloat16)
    widened = stream.astype(jnp.float32)
    normed = widened * lax.rsqrt(lax.optimization_barrier(jnp.mean(widened * widened, axis=-1, keepdims=True)) + 1e-06)
    scored = lax.optimization_barrier(jnp.sum(normed * (norm_gain * value_head)[None, :], axis=-1))
    scored = jnp.where(positions < valid_upto, scored, 0.0)
    return (stream, scored)
```

```python
import functools
import math

import jax
import jax.numpy as jnp
from jax import lax
from jax.experimental import pallas as pl
from jax.experimental.pallas import tpu as pltpu
from jax.sharding import PartitionSpec as P

HEAD_DIM = 128
NEG_BIG = -1e30
CORES = 2
ROWS_Y = 2
PLANE = CORES * ROWS_Y

W_UP, W_DOWN, W_Y, W_X, W_CORE, W_CORE_X, KV_UP, KV_Y, KV_CORE = range(9)


def kernel(
    planes,
    valid_ref,
    q_hbm,
    key_hbm,
    value_hbm,
    residual_hbm,
    weight_hbm,
    gain_ref,
    stream_ref,
    values_ref,
    q_ref,
    kv,
    weight,
    residual,
    attended,
    row_max,
    row_sum,
    out_sum,
    send,
    recv,
    local,
):
    league = lax.axis_index("league")
    me = lax.axis_index("seq")
    z = me // PLANE
    y = (me // CORES) % ROWS_Y
    c = me % CORES
    tok, width = residual.shape
    share = (width * 11 // 28) // 128 * 128
    whole = pl.ds(0, width)

    def slot(zp, yp, cp):
        return zp * PLANE + yp * CORES + cp

    def near(dz=0, fy=False, fc=False):
        yy = 1 - y if fy else y
        cc = 1 - c if fc else c
        return (league, slot(z + dz, yy, cc))

    side = league % 2
    over_x = (league + 1 - 2 * side, me)
    mine = pl.ds(pl.multiple_of(side * share, 128), width - share)
    given = pl.ds(pl.multiple_of(side * (width - share), 128), share)
    taken = pl.ds(pl.multiple_of((1 - side) * (width - share), 128), share)

    def move(kind, zp, yp, cp, target, columns=None):
        index = zp * ROWS_Y + yp
        if kind in (KV_UP, KV_Y, KV_CORE):
            ref = kv.at[slot(zp, yp, cp)]
        else:
            ref = weight.at[slot(zp, yp, cp), :, columns]
        return pltpu.make_async_remote_copy(
            src_ref=ref,
            dst_ref=ref,
            send_sem=send.at[kind, index],
            recv_sem=recv.at[kind, index],
            device_id=target,
            device_id_type=pl.DeviceIdType.MESH,
        )

    other_core = near(fc=True)
    other_y = near(fy=True)
    up = (league, jnp.minimum(me + PLANE, planes * PLANE - 1))
    down = (league, jnp.maximum(me - PLANE, 0))
    has_up = z < planes - 1
    has_down = z > 0

    loads = [
        pltpu.make_async_copy(key_hbm, kv.at[me, :, pl.ds(0, key_hbm.shape[1])], local.at[0]),
        pltpu.make_async_copy(
            value_hbm, kv.at[me, :, pl.ds(key_hbm.shape[1], key_hbm.shape[1])], local.at[1]
        ),
        pltpu.make_async_copy(weight_hbm, weight.at[me], local.at[2]),
        pltpu.make_async_copy(q_hbm, q_ref, local.at[3]),
        pltpu.make_async_copy(residual_hbm, residual, local.at[4]),
    ]
    for load in loads:
        load.start()

    barrier = pltpu.get_barrier_semaphore()

    def greet(target):
        pl.semaphore_signal(
            barrier, inc=1, device_id=target, device_id_type=pl.DeviceIdType.MESH
        )

    greet(over_x)
    greet(other_y)
    greet(other_core)
    pl.when(has_up)(lambda: greet(up))
    pl.when(has_down)(lambda: greet(down))
    pl.semaphore_wait(barrier, 3 + has_up.astype(jnp.int32) + has_down.astype(jnp.int32))

    def spread_kv(zp):
        pl.when(has_up)(lambda: move(KV_UP, zp, y, c, up).start())
        move(KV_Y, zp, y, c, other_y).start()
        move(KV_CORE, zp, y, c, other_core).start()

    loads[0].wait()
    loads[1].wait()
    spread_kv(z)
    loads[2].wait()
    pl.when(has_down)(lambda: move(W_DOWN, z, y, c, down, mine).start())

    def kv_round(r, carry):
        @pl.when(jnp.logical_and(r >= 1, z - r >= 0))
        def _():
            move(KV_UP, z - r, y, c, up).wait_recv()
            spread_kv(z - r)

        @pl.when(jnp.logical_and(r >= 1, z - r + 1 >= 0))
        def _():
            move(KV_Y, z - r + 1, 1 - y, c, other_y).wait_recv()
            move(KV_CORE, z - r + 1, 1 - y, c, other_core).start()

        return carry

    lax.fori_loop(0, planes + 1, kv_round, 0)

    pl.when(has_up)(lambda: move(W_UP, z, y, c, up, mine).start())
    move(W_Y, z, y, c, other_y, mine).start()
    move(W_CORE, z, y, c, other_core, whole).start()
    loads[3].wait()

    heads = q_ref.shape[1] // HEAD_DIM
    groups = key_hbm.shape[1] // HEAD_DIM
    factor = HEAD_DIM ** (-0.5) * math.log2(math.e)
    row_max[...] = jnp.full(row_max.shape, NEG_BIG, jnp.float32)
    row_sum[...] = jnp.zeros(row_sum.shape, jnp.float32)
    out_sum[...] = jnp.zeros(out_sum.shape, jnp.float32)

    def attend(zp):
        for yp in (y, 1 - y):
            move(KV_CORE, zp, yp, 1 - c, other_core).wait_recv()
        keys = PLANE * tok
        query_pos = me * tok + lax.broadcasted_iota(jnp.int32, (tok, keys), 0)
        key_pos = zp * keys + lax.broadcasted_iota(jnp.int32, (tok, keys), 1)
        allowed = key_pos <= query_pos

        def one_head(h, carry):
            g = h // (heads // groups)
            q = q_ref[:, pl.ds(pl.multiple_of(h * HEAD_DIM, HEAD_DIM), HEAD_DIM)]
            at = pl.ds(zp * PLANE, PLANE)
            k = kv[at, :, pl.ds(pl.multiple_of(g * HEAD_DIM, HEAD_DIM), HEAD_DIM)]
            v = kv[at, :, pl.ds(pl.multiple_of((groups + g) * HEAD_DIM, HEAD_DIM), HEAD_DIM)]
            k = k.reshape(keys, HEAD_DIM)
            v = v.reshape(keys, HEAD_DIM)
            scores = lax.dot_general(
                q, k, (((1,), (1,)), ((), ())), preferred_element_type=jnp.float32
            )
            scores = jnp.where(allowed, scores * factor, NEG_BIG)
            old_max = row_max[h]
            new_max = jnp.maximum(old_max, jnp.max(scores, axis=1, keepdims=True))
            shrink = jnp.exp2(old_max - new_max)
            weights = jnp.exp2(scores - new_max)
            row_max[h] = new_max
            row_sum[h] = row_sum[h] * shrink + jnp.sum(weights, axis=1, keepdims=True)
            out_sum[h] = out_sum[h] * shrink + jnp.dot(
                weights.astype(jnp.bfloat16), v, preferred_element_type=jnp.float32
            )
            return carry

        lax.fori_loop(0, heads, one_head, 0)

    def onward(zp, yp):
        move(W_X, zp, yp, c, over_x, given).start()
        move(W_CORE, zp, yp, c, other_core, mine).start()

    def each_plane(r, body):
        pl.when(jnp.logical_and(r >= 0, z - r >= 0))(lambda: body(z - r))
        pl.when(jnp.logical_and(r >= 1, z + r < planes))(lambda: body(z + r))

    def weight_round(r, carry):
        @pl.when(jnp.logical_and(r >= 1, z - r >= 0))
        def _():
            move(W_UP, z - r, y, c, up, mine).wait_recv()
            pl.when(has_up)(lambda: move(W_UP, z - r, y, c, up, mine).start())
            move(W_Y, z - r, y, c, other_y, mine).start()
            onward(z - r, y)

        @pl.when(jnp.logical_and(r >= 1, z + r < planes))
        def _():
            move(W_DOWN, z + r, y, c, down, mine).wait_recv()
            pl.when(has_down)(lambda: move(W_DOWN, z + r, y, c, down, mine).start())
            move(W_Y, z + r, y, c, other_y, mine).start()
            onward(z + r, y)

        def from_y(zp):
            move(W_Y, zp, 1 - y, c, other_y, mine).wait_recv()
            onward(zp, 1 - y)

        each_plane(r - 1, from_y)

        def from_x(zp):
            def one(yp):
                move(W_X, zp, yp, c, over_x, taken).wait_recv()
                move(W_CORE_X, zp, yp, c, other_core, taken).start()

            pl.when(zp != z)(lambda: one(y))
            one(1 - y)

        each_plane(r - 2, from_x)
        pl.when(z - r >= 0)(lambda: attend(z - r))
        return carry

    lax.fori_loop(0, planes + 2, weight_round, 0)

    valid = valid_ref[0]
    rows = me * tok + lax.broadcasted_iota(jnp.int32, (tok, 1), 0)
    row_ok = rows < valid
    for h in range(heads):
        mixed = jnp.where(row_ok, out_sum[h] / jnp.where(row_ok, row_sum[h], 1.0), 0.0)
        attended[:, h * HEAD_DIM : (h + 1) * HEAD_DIM] = mixed.astype(jnp.bfloat16)
    loads[4].wait()

    def arrived(zp, carry):
        for yp in (y, 1 - y):
            own = jnp.logical_and(zp == z, yp == y)

            @pl.when(own)
            def _():
                move(W_CORE, zp, yp, 1 - c, other_core, whole).wait_recv()

            @pl.when(jnp.logical_not(own))
            def _():
                move(W_CORE, zp, yp, 1 - c, other_core, mine).wait_recv()
                move(W_CORE_X, zp, yp, 1 - c, other_core, taken).wait_recv()

        return carry

    lax.fori_loop(0, planes, arrived, 0)

    tile = math.gcd(width, 512)
    depth = weight.shape[1]
    count = weight.shape[0]

    def one_tile(t, carry):
        squares, dots = carry
        cols = pl.ds(pl.multiple_of(t * tile, tile), tile)
        if depth % 16 == 0:
            projected = jnp.dot(
                attended[...],
                weight[:, :, cols].reshape(count * depth, tile),
                preferred_element_type=jnp.float32,
            )
        else:
            projected = jnp.zeros((tok, tile), jnp.float32)
            for s in range(count):
                projected += jnp.dot(
                    attended[:, s * depth : (s + 1) * depth],
                    weight[s, :, cols],
                    preferred_element_type=jnp.float32,
                )
        stream = (residual[:, cols].astype(jnp.float32) + projected).astype(jnp.bfloat16)
        stream_ref[:, cols] = stream
        widened = stream.astype(jnp.float32)
        squares += jnp.sum(widened * widened, axis=1, keepdims=True)
        dots += jnp.sum(widened * gain_ref[:, cols], axis=1, keepdims=True)
        return squares, dots

    zero = jnp.zeros((tok, 1), jnp.float32)
    squares, dots = lax.fori_loop(0, width // tile, one_tile, (zero, zero))
    scored = dots * lax.rsqrt(squares / width + 1e-06)
    values_ref[...] = jnp.where(row_ok, scored, 0.0)

    def drain(zp, carry):
        @pl.when(zp <= z)
        def _():
            pl.when(has_up)(lambda: move(KV_UP, zp, y, c, up).wait_send())
            pl.when(has_up)(lambda: move(W_UP, zp, y, c, up, mine).wait_send())
            move(KV_Y, zp, y, c, other_y).wait_send()
            move(KV_CORE, zp, y, c, other_core).wait_send()
            move(KV_CORE, zp, 1 - y, c, other_core).wait_send()

        @pl.when(jnp.logical_and(zp >= z, has_down))
        def _():
            move(W_DOWN, zp, y, c, down, mine).wait_send()

        move(W_Y, zp, y, c, other_y, mine).wait_send()

        def sent(yp):
            move(W_X, zp, yp, c, over_x, given).wait_send()
            move(W_CORE, zp, yp, c, other_core, mine).wait_send()
            move(W_CORE_X, zp, yp, c, other_core, taken).wait_send()

        sent(1 - y)
        pl.when(zp != z)(lambda: sent(y))
        pl.when(zp == z)(lambda: move(W_CORE, zp, y, c, other_core, whole).wait_send())
        return carry

    lax.fori_loop(0, planes, drain, 0)


def per_device(
    devices,
    queries,
    key_rows,
    value_rows,
    residual,
    out_weight,
    norm_gain,
    value_head,
    valid_length,
):
    tok, q_width = queries.shape
    width = residual.shape[1]
    heads = q_width // HEAD_DIM
    planes = devices // PLANE
    any_space = pl.BlockSpec(memory_space=pl.ANY)
    vmem = pl.BlockSpec(memory_space=pltpu.VMEM)
    stream, scored = pl.pallas_call(
        functools.partial(kernel, planes),
        name="critic_block",
        out_shape=(
            jax.ShapeDtypeStruct((tok, width), jnp.bfloat16),
            jax.ShapeDtypeStruct((tok, 1), jnp.float32),
        ),
        in_specs=[pl.BlockSpec(memory_space=pltpu.SMEM)] + [any_space] * 5 + [vmem],
        out_specs=(vmem, vmem),
        scratch_shapes=[
            pltpu.VMEM((tok, q_width), jnp.bfloat16),
            pltpu.VMEM((devices, tok, 2 * key_rows.shape[1]), jnp.bfloat16),
            pltpu.VMEM((devices,) + out_weight.shape, jnp.bfloat16),
            pltpu.VMEM((tok, width), jnp.bfloat16),
            pltpu.VMEM((tok, q_width), jnp.bfloat16),
            pltpu.VMEM((heads, tok, 1), jnp.float32),
            pltpu.VMEM((heads, tok, 1), jnp.float32),
            pltpu.VMEM((heads, tok, HEAD_DIM), jnp.float32),
            pltpu.SemaphoreType.DMA((9, ROWS_Y * planes)),
            pltpu.SemaphoreType.DMA((9, ROWS_Y * planes)),
            pltpu.SemaphoreType.DMA((5,)),
        ],
        compiler_params=pltpu.CompilerParams(
            collective_id=0, has_side_effects=True, vmem_limit_bytes=60 * 1024 * 1024
        ),
    )(
        valid_length,
        queries,
        key_rows,
        value_rows,
        residual,
        out_weight,
        (norm_gain * value_head)[None, :],
    )
    return stream, scored[:, 0]


def solution(mesh):
    rows = P(("league", "seq"), None)
    return jax.shard_map(
        functools.partial(per_device, mesh.shape["seq"]),
        mesh=mesh,
        in_specs=(rows, rows, rows, rows, P("seq", None), P(), P(), P("league")),
        out_specs=(rows, P(("league", "seq"))),
        check_vma=False,
    )
```

```python
import functools
import math

import jax
import jax.numpy as jnp
from jax import lax
from jax.experimental import pallas as pl
from jax.experimental.pallas import tpu as pltpu
from jax.sharding import PartitionSpec as P

HEAD_DIM = 128
NEG_BIG = -1e30
CORES = 2
ROWS_Y = 2
PLANE = CORES * ROWS_Y

W_UP, W_DOWN, W_Y, W_X, W_CORE, W_CORE_X, KV_UP, KV_Y, KV_CORE = range(9)


def kernel(
    planes,
    valid_ref,
    q_hbm,
    key_hbm,
    value_hbm,
    residual_hbm,
    weight_hbm,
    gain_ref,
    stream_ref,
    values_ref,
    q_ref,
    kv,
    weight,
    residual,
    attended,
    projected,
    row_max,
    row_sum,
    out_sum,
    send,
    recv,
    local,
):
    league = lax.axis_index("league")
    me = lax.axis_index("seq")
    z = me // PLANE
    y = (me // CORES) % ROWS_Y
    c = me % CORES
    tok, width = residual.shape
    share = (width * 11 // 28) // 128 * 128
    whole = pl.ds(0, width)

    def slot(zp, yp, cp):
        return zp * PLANE + yp * CORES + cp

    def near(dz=0, fy=False, fc=False):
        yy = 1 - y if fy else y
        cc = 1 - c if fc else c
        return (league, slot(z + dz, yy, cc))

    side = league % 2
    over_x = (league + 1 - 2 * side, me)
    mine = pl.ds(pl.multiple_of(side * share, 128), width - share)
    given = pl.ds(pl.multiple_of(side * (width - share), 128), share)
    taken = pl.ds(pl.multiple_of((1 - side) * (width - share), 128), share)

    def move(kind, zp, yp, cp, target, columns=None):
        index = zp * ROWS_Y + yp
        if kind in (KV_UP, KV_Y, KV_CORE):
            ref = kv.at[slot(zp, yp, cp)]
        else:
            ref = weight.at[slot(zp, yp, cp), :, columns]
        return pltpu.make_async_remote_copy(
            src_ref=ref,
            dst_ref=ref,
            send_sem=send.at[kind, index],
            recv_sem=recv.at[kind, index],
            device_id=target,
            device_id_type=pl.DeviceIdType.MESH,
        )

    other_core = near(fc=True)
    other_y = near(fy=True)
    up = (league, jnp.minimum(me + PLANE, planes * PLANE - 1))
    down = (league, jnp.maximum(me - PLANE, 0))
    has_up = z < planes - 1
    has_down = z > 0

    loads = [
        pltpu.make_async_copy(key_hbm, kv.at[me, :, pl.ds(0, key_hbm.shape[1])], local.at[0]),
        pltpu.make_async_copy(
            value_hbm, kv.at[me, :, pl.ds(key_hbm.shape[1], key_hbm.shape[1])], local.at[1]
        ),
        pltpu.make_async_copy(weight_hbm, weight.at[me], local.at[2]),
        pltpu.make_async_copy(q_hbm, q_ref, local.at[3]),
        pltpu.make_async_copy(residual_hbm, residual, local.at[4]),
    ]
    for load in loads:
        load.start()

    barrier = pltpu.get_barrier_semaphore()

    def greet(target):
        pl.semaphore_signal(
            barrier, inc=1, device_id=target, device_id_type=pl.DeviceIdType.MESH
        )

    greet(over_x)
    greet(other_y)
    greet(other_core)
    pl.when(has_up)(lambda: greet(up))
    pl.when(has_down)(lambda: greet(down))
    pl.semaphore_wait(barrier, 3 + has_up.astype(jnp.int32) + has_down.astype(jnp.int32))

    def spread_kv(zp):
        pl.when(has_up)(lambda: move(KV_UP, zp, y, c, up).start())
        move(KV_Y, zp, y, c, other_y).start()
        move(KV_CORE, zp, y, c, other_core).start()

    loads[0].wait()
    loads[1].wait()
    pl.when(has_up)(lambda: move(KV_UP, z, y, c, up).start())
    move(KV_CORE, z, y, c, other_core).start()
    loads[2].wait()
    move(W_Y, z, y, c, other_y, mine).start()
    pl.when(has_down)(lambda: move(W_DOWN, z, y, c, down, mine).start())
    pl.when(has_up)(lambda: move(W_UP, z, y, c, up, mine).start())
    move(KV_Y, z, y, c, other_y).start()
    move(W_CORE, z, y, c, other_core, whole).start()
    loads[3].wait()
    loads[4].wait()

    heads = q_ref.shape[1] // HEAD_DIM
    groups = key_hbm.shape[1] // HEAD_DIM
    factor = HEAD_DIM ** (-0.5) * math.log2(math.e)
    row_max[...] = jnp.full(row_max.shape, NEG_BIG, jnp.float32)
    row_sum[...] = jnp.zeros(row_sum.shape, jnp.float32)
    out_sum[...] = jnp.zeros(out_sum.shape, jnp.float32)

    def attend(zp):
        for yp in (y, 1 - y):
            move(KV_CORE, zp, yp, 1 - c, other_core).wait_recv()
        keys = PLANE * tok
        query_pos = me * tok + lax.broadcasted_iota(jnp.int32, (tok, keys), 0)
        key_pos = zp * keys + lax.broadcasted_iota(jnp.int32, (tok, keys), 1)
        allowed = key_pos <= query_pos

        def one_head(h, carry):
            g = h // (heads // groups)
            q = q_ref[:, pl.ds(pl.multiple_of(h * HEAD_DIM, HEAD_DIM), HEAD_DIM)]
            at = pl.ds(zp * PLANE, PLANE)
            k = kv[at, :, pl.ds(pl.multiple_of(g * HEAD_DIM, HEAD_DIM), HEAD_DIM)]
            v = kv[at, :, pl.ds(pl.multiple_of((groups + g) * HEAD_DIM, HEAD_DIM), HEAD_DIM)]
            k = k.reshape(keys, HEAD_DIM)
            v = v.reshape(keys, HEAD_DIM)
            scores = lax.dot_general(
                q, k, (((1,), (1,)), ((), ())), preferred_element_type=jnp.float32
            )
            scores = jnp.where(allowed, scores * factor, NEG_BIG)
            old_max = row_max[h]
            new_max = jnp.maximum(old_max, jnp.max(scores, axis=1, keepdims=True))
            shrink = jnp.exp2(old_max - new_max)
            weights = jnp.exp2(scores - new_max)
            row_max[h] = new_max
            row_sum[h] = row_sum[h] * shrink + jnp.sum(weights, axis=1, keepdims=True)
            out_sum[h] = out_sum[h] * shrink + jnp.dot(
                weights.astype(jnp.bfloat16), v, preferred_element_type=jnp.float32
            )
            return carry

        lax.fori_loop(0, heads, one_head, 0)

    def onward(zp, yp):
        move(W_X, zp, yp, c, over_x, given).start()
        move(W_CORE, zp, yp, c, other_core, mine).start()

    def each_plane(r, body):
        pl.when(jnp.logical_and(r >= 0, z - r >= 0))(lambda: body(z - r))
        pl.when(jnp.logical_and(r >= 1, z + r < planes))(lambda: body(z + r))

    def arrived(zp):
        for yp in (y, 1 - y):
            own = jnp.logical_and(zp == z, yp == y)

            @pl.when(own)
            def _():
                move(W_CORE, zp, yp, 1 - c, other_core, whole).wait_recv()

            @pl.when(jnp.logical_not(own))
            def _():
                move(W_CORE, zp, yp, 1 - c, other_core, mine).wait_recv()
                move(W_CORE_X, zp, yp, 1 - c, other_core, taken).wait_recv()

    tile = math.gcd(width, 512)
    depth = weight.shape[1]

    def project(zp):
        arrived(zp)

        def one_tile(t, carry):
            cols = pl.ds(pl.multiple_of(t * tile, tile), tile)
            rows = attended[zp]
            if depth % 16 == 0:
                block = weight[pl.ds(zp * PLANE, PLANE), :, cols]
                projected[:, cols] += jnp.dot(
                    rows,
                    block.reshape(PLANE * depth, tile),
                    preferred_element_type=jnp.float32,
                )
            else:
                for i in range(PLANE):
                    projected[:, cols] += jnp.dot(
                        rows[:, i * depth : (i + 1) * depth],
                        weight[zp * PLANE + i, :, cols],
                        preferred_element_type=jnp.float32,
                    )
            return carry

        lax.fori_loop(0, width // tile, one_tile, 0)

    valid = valid_ref[0]
    row_ok = me * tok + lax.broadcasted_iota(jnp.int32, (tok, 1), 0) < valid

    def finish_attention():
        parts = []
        for h in range(heads):
            mixed = out_sum[h] / jnp.where(row_ok, row_sum[h], 1.0)
            parts.append(jnp.where(row_ok, mixed, 0.0).astype(jnp.bfloat16))
        joined = jnp.concatenate(parts, axis=1)
        for zp in range(planes):
            attended[zp] = joined[:, zp * PLANE * depth : (zp + 1) * PLANE * depth]
        projected[...] = residual[...].astype(jnp.float32)

    def weight_round(r, carry):
        @pl.when(jnp.logical_and(r >= 1, z - r >= 0))
        def _():
            move(KV_UP, z - r, y, c, up).wait_recv()
            spread_kv(z - r)

        @pl.when(jnp.logical_and(r >= 1, z - r >= 0))
        def _():
            move(W_UP, z - r, y, c, up, mine).wait_recv()
            pl.when(has_up)(lambda: move(W_UP, z - r, y, c, up, mine).start())
            move(W_Y, z - r, y, c, other_y, mine).start()
            onward(z - r, y)

        @pl.when(jnp.logical_and(r >= 1, z + r < planes))
        def _():
            move(W_DOWN, z + r, y, c, down, mine).wait_recv()
            pl.when(has_down)(lambda: move(W_DOWN, z + r, y, c, down, mine).start())
            move(W_Y, z + r, y, c, other_y, mine).start()
            onward(z + r, y)

        def from_y(zp):
            move(W_Y, zp, 1 - y, c, other_y, mine).wait_recv()
            onward(zp, 1 - y)

        each_plane(r - 1, from_y)

        @pl.when(jnp.logical_and(r >= 1, z - r + 1 >= 0))
        def _():
            move(KV_Y, z - r + 1, 1 - y, c, other_y).wait_recv()
            move(KV_CORE, z - r + 1, 1 - y, c, other_core).start()

        def from_x(zp):
            def one(yp):
                move(W_X, zp, yp, c, over_x, taken).wait_recv()
                move(W_CORE_X, zp, yp, c, other_core, taken).start()

            pl.when(zp != z)(lambda: one(y))
            one(1 - y)

        each_plane(r - 2, from_x)
        pl.when(jnp.logical_and(r >= 1, z - r + 1 >= 0))(lambda: attend(z - r + 1))

        @pl.when(r == planes)
        def _():
            finish_attention()

            def near_plane(d, carry):
                each_plane(d, project)
                return carry

            lax.fori_loop(0, planes - 1, near_plane, 0)

        return carry

    lax.fori_loop(0, planes + 2, weight_round, 0)
    each_plane(planes - 1, project)

    def finish_tile(t, carry):
        squares, dots = carry
        cols = pl.ds(pl.multiple_of(t * tile, tile), tile)
        stream = projected[:, cols].astype(jnp.bfloat16)
        stream_ref[:, cols] = stream
        widened = stream.astype(jnp.float32)
        squares += jnp.sum(widened * widened, axis=1, keepdims=True)
        dots += jnp.sum(widened * gain_ref[:, cols], axis=1, keepdims=True)
        return squares, dots

    zero = jnp.zeros((tok, 1), jnp.float32)
    squares, dots = lax.fori_loop(0, width // tile, finish_tile, (zero, zero))
    scored = dots * lax.rsqrt(squares / width + 1e-06)
    values_ref[...] = jnp.where(row_ok, scored, 0.0)

    def drain(zp, carry):
        @pl.when(zp <= z)
        def _():
            pl.when(has_up)(lambda: move(KV_UP, zp, y, c, up).wait_send())
            pl.when(has_up)(lambda: move(W_UP, zp, y, c, up, mine).wait_send())
            move(KV_Y, zp, y, c, other_y).wait_send()
            move(KV_CORE, zp, y, c, other_core).wait_send()
            move(KV_CORE, zp, 1 - y, c, other_core).wait_send()

        @pl.when(jnp.logical_and(zp >= z, has_down))
        def _():
            move(W_DOWN, zp, y, c, down, mine).wait_send()

        move(W_Y, zp, y, c, other_y, mine).wait_send()

        def sent(yp):
            move(W_X, zp, yp, c, over_x, given).wait_send()
            move(W_CORE, zp, yp, c, other_core, mine).wait_send()
            move(W_CORE_X, zp, yp, c, other_core, taken).wait_send()

        sent(1 - y)
        pl.when(zp != z)(lambda: sent(y))
        pl.when(zp == z)(lambda: move(W_CORE, zp, y, c, other_core, whole).wait_send())
        return carry

    lax.fori_loop(0, planes, drain, 0)


def per_device(
    devices,
    queries,
    key_rows,
    value_rows,
    residual,
    out_weight,
    norm_gain,
    value_head,
    valid_length,
):
    tok, q_width = queries.shape
    width = residual.shape[1]
    heads = q_width // HEAD_DIM
    planes = devices // PLANE
    any_space = pl.BlockSpec(memory_space=pl.ANY)
    vmem = pl.BlockSpec(memory_space=pltpu.VMEM)
    stream, scored = pl.pallas_call(
        functools.partial(kernel, planes),
        name="critic_block",
        out_shape=(
            jax.ShapeDtypeStruct((tok, width), jnp.bfloat16),
            jax.ShapeDtypeStruct((tok, 1), jnp.float32),
        ),
        in_specs=[pl.BlockSpec(memory_space=pltpu.SMEM)] + [any_space] * 5 + [vmem],
        out_specs=(vmem, vmem),
        scratch_shapes=[
            pltpu.VMEM((tok, q_width), jnp.bfloat16),
            pltpu.VMEM((devices, tok, 2 * key_rows.shape[1]), jnp.bfloat16),
            pltpu.VMEM((devices,) + out_weight.shape, jnp.bfloat16),
            pltpu.VMEM((tok, width), jnp.bfloat16),
            pltpu.VMEM((planes, tok, q_width // planes), jnp.bfloat16),
            pltpu.VMEM((tok, width), jnp.float32),
            pltpu.VMEM((heads, tok, 1), jnp.float32),
            pltpu.VMEM((heads, tok, 1), jnp.float32),
            pltpu.VMEM((heads, tok, HEAD_DIM), jnp.float32),
            pltpu.SemaphoreType.DMA((9, ROWS_Y * planes)),
            pltpu.SemaphoreType.DMA((9, ROWS_Y * planes)),
            pltpu.SemaphoreType.DMA((5,)),
        ],
        compiler_params=pltpu.CompilerParams(
            collective_id=0, has_side_effects=True, vmem_limit_bytes=60 * 1024 * 1024
        ),
    )(
        valid_length,
        queries,
        key_rows,
        value_rows,
        residual,
        out_weight,
        (norm_gain * value_head)[None, :],
    )
    return stream, scored[:, 0]


def solution(mesh):
    rows = P(("league", "seq"), None)
    return jax.shard_map(
        functools.partial(per_device, mesh.shape["seq"]),
        mesh=mesh,
        in_specs=(rows, rows, rows, rows, P("seq", None), P(), P(), P("league")),
        out_specs=(rows, P(("league", "seq"))),
        check_vma=False,
    )
```

```python
import functools
import math

import jax
import jax.numpy as jnp
from jax import lax
from jax.experimental import pallas as pl
from jax.experimental.pallas import tpu as pltpu
from jax.sharding import PartitionSpec as P

HEAD_DIM = 128
NEG_BIG = -1e30
CORES = 2
ROWS_Y = 2
PLANE = CORES * ROWS_Y

W_UP, W_DOWN, W_Y, W_X, W_CORE, W_CORE_X, KV_UP, KV_Y, KV_CORE = range(9)


def kernel(
    planes,
    valid_ref,
    q_hbm,
    key_hbm,
    value_hbm,
    residual_hbm,
    weight_hbm,
    gain_ref,
    stream_ref,
    values_ref,
    q_ref,
    kv,
    weight,
    residual,
    attended,
    projected,
    row_max,
    row_sum,
    out_sum,
    send,
    recv,
    local,
):
    league = lax.axis_index("league")
    me = lax.axis_index("seq")
    z = me // PLANE
    y = (me // CORES) % ROWS_Y
    c = me % CORES
    tok, width = residual.shape
    share = (width * 12 // 28) // 128 * 128
    whole = pl.ds(0, width)

    def slot(zp, yp, cp):
        return zp * PLANE + yp * CORES + cp

    def near(dz=0, fy=False, fc=False):
        yy = 1 - y if fy else y
        cc = 1 - c if fc else c
        return (league, slot(z + dz, yy, cc))

    side = league % 2
    over_x = (league + 1 - 2 * side, me)
    mine = pl.ds(pl.multiple_of(side * share, 128), width - share)
    given = pl.ds(pl.multiple_of(side * (width - share), 128), share)
    taken = pl.ds(pl.multiple_of((1 - side) * (width - share), 128), share)

    def move(kind, zp, yp, cp, target, columns=None):
        index = zp * ROWS_Y + yp
        if kind in (KV_UP, KV_Y, KV_CORE):
            ref = kv.at[slot(zp, yp, cp)]
        else:
            ref = weight.at[slot(zp, yp, cp), :, columns]
        return pltpu.make_async_remote_copy(
            src_ref=ref,
            dst_ref=ref,
            send_sem=send.at[kind, index],
            recv_sem=recv.at[kind, index],
            device_id=target,
            device_id_type=pl.DeviceIdType.MESH,
        )

    other_core = near(fc=True)
    other_y = near(fy=True)
    up = (league, jnp.minimum(me + PLANE, planes * PLANE - 1))
    down = (league, jnp.maximum(me - PLANE, 0))
    has_up = z < planes - 1
    has_down = z > 0

    loads = [
        pltpu.make_async_copy(key_hbm, kv.at[me, :, pl.ds(0, key_hbm.shape[1])], local.at[0]),
        pltpu.make_async_copy(
            value_hbm, kv.at[me, :, pl.ds(key_hbm.shape[1], key_hbm.shape[1])], local.at[1]
        ),
        pltpu.make_async_copy(weight_hbm, weight.at[me], local.at[2]),
        pltpu.make_async_copy(q_hbm, q_ref, local.at[3]),
        pltpu.make_async_copy(residual_hbm, residual, local.at[4]),
    ]
    for load in loads:
        load.start()

    barrier = pltpu.get_barrier_semaphore()

    def greet(target):
        pl.semaphore_signal(
            barrier, inc=1, device_id=target, device_id_type=pl.DeviceIdType.MESH
        )

    greet(over_x)
    greet(other_y)
    greet(other_core)
    pl.when(has_up)(lambda: greet(up))
    pl.when(has_down)(lambda: greet(down))
    pl.semaphore_wait(barrier, 3 + has_up.astype(jnp.int32) + has_down.astype(jnp.int32))

    def spread_kv(zp):
        pl.when(has_up)(lambda: move(KV_UP, zp, y, c, up).start())
        move(KV_Y, zp, y, c, other_y).start()
        move(KV_CORE, zp, y, c, other_core).start()

    loads[0].wait()
    loads[1].wait()
    pl.when(has_up)(lambda: move(KV_UP, z, y, c, up).start())
    move(KV_CORE, z, y, c, other_core).start()
    loads[2].wait()
    move(W_Y, z, y, c, other_y, mine).start()
    pl.when(has_down)(lambda: move(W_DOWN, z, y, c, down, mine).start())
    pl.when(has_up)(lambda: move(W_UP, z, y, c, up, mine).start())
    move(KV_Y, z, y, c, other_y).start()
    move(W_CORE, z, y, c, other_core, whole).start()
    loads[3].wait()
    loads[4].wait()

    heads = q_ref.shape[1] // HEAD_DIM
    groups = key_hbm.shape[1] // HEAD_DIM
    factor = HEAD_DIM ** (-0.5) * math.log2(math.e)
    row_max[...] = jnp.full(row_max.shape, NEG_BIG, jnp.float32)
    row_sum[...] = jnp.zeros(row_sum.shape, jnp.float32)
    out_sum[...] = jnp.zeros(out_sum.shape, jnp.float32)

    def attend(zp):
        for yp in (y, 1 - y):
            move(KV_CORE, zp, yp, 1 - c, other_core).wait_recv()
        keys = PLANE * tok
        query_pos = me * tok + lax.broadcasted_iota(jnp.int32, (tok, keys), 0)
        key_pos = zp * keys + lax.broadcasted_iota(jnp.int32, (tok, keys), 1)
        allowed = key_pos <= query_pos

        def one_head(h, carry):
            g = h // (heads // groups)
            q = q_ref[:, pl.ds(pl.multiple_of(h * HEAD_DIM, HEAD_DIM), HEAD_DIM)]
            at = pl.ds(zp * PLANE, PLANE)
            k = kv[at, :, pl.ds(pl.multiple_of(g * HEAD_DIM, HEAD_DIM), HEAD_DIM)]
            v = kv[at, :, pl.ds(pl.multiple_of((groups + g) * HEAD_DIM, HEAD_DIM), HEAD_DIM)]
            k = k.reshape(keys, HEAD_DIM)
            v = v.reshape(keys, HEAD_DIM)
            scores = lax.dot_general(
                q, k, (((1,), (1,)), ((), ())), preferred_element_type=jnp.float32
            )
            scores = jnp.where(allowed, scores * factor, NEG_BIG)
            old_max = row_max[h]
            new_max = jnp.maximum(old_max, jnp.max(scores, axis=1, keepdims=True))
            shrink = jnp.exp2(old_max - new_max)
            weights = jnp.exp2(scores - new_max)
            row_max[h] = new_max
            row_sum[h] = row_sum[h] * shrink + jnp.sum(weights, axis=1, keepdims=True)
            out_sum[h] = out_sum[h] * shrink + jnp.dot(
                weights.astype(jnp.bfloat16), v, preferred_element_type=jnp.float32
            )
            return carry

        lax.fori_loop(0, heads, one_head, 0)

    def onward(zp, yp):
        move(W_X, zp, yp, c, over_x, given).start()
        move(W_CORE, zp, yp, c, other_core, mine).start()

    def each_plane(r, body):
        pl.when(jnp.logical_and(r >= 0, z - r >= 0))(lambda: body(z - r))
        pl.when(jnp.logical_and(r >= 1, z + r < planes))(lambda: body(z + r))

    def arrived(zp):
        for yp in (y, 1 - y):
            own = jnp.logical_and(zp == z, yp == y)

            @pl.when(own)
            def _():
                move(W_CORE, zp, yp, 1 - c, other_core, whole).wait_recv()

            @pl.when(jnp.logical_not(own))
            def _():
                move(W_CORE, zp, yp, 1 - c, other_core, mine).wait_recv()
                move(W_CORE_X, zp, yp, 1 - c, other_core, taken).wait_recv()

    tile = math.gcd(width, 512)
    depth = weight.shape[1]

    def project(zp):
        arrived(zp)

        def one_tile(t, carry):
            cols = pl.ds(pl.multiple_of(t * tile, tile), tile)
            rows = attended[zp]
            if depth % 16 == 0:
                block = weight[pl.ds(zp * PLANE, PLANE), :, cols]
                projected[:, cols] += jnp.dot(
                    rows,
                    block.reshape(PLANE * depth, tile),
                    preferred_element_type=jnp.float32,
                )
            else:
                for i in range(PLANE):
                    projected[:, cols] += jnp.dot(
                        rows[:, i * depth : (i + 1) * depth],
                        weight[zp * PLANE + i, :, cols],
                        preferred_element_type=jnp.float32,
                    )
            return carry

        lax.fori_loop(0, width // tile, one_tile, 0)

    valid = valid_ref[0]
    row_ok = me * tok + lax.broadcasted_iota(jnp.int32, (tok, 1), 0) < valid

    def finish_attention():
        parts = []
        for h in range(heads):
            mixed = out_sum[h] / jnp.where(row_ok, row_sum[h], 1.0)
            parts.append(jnp.where(row_ok, mixed, 0.0).astype(jnp.bfloat16))
        joined = jnp.concatenate(parts, axis=1)
        for zp in range(planes):
            attended[zp] = joined[:, zp * PLANE * depth : (zp + 1) * PLANE * depth]
        projected[...] = residual[...].astype(jnp.float32)

    def weight_round(r, carry):
        @pl.when(jnp.logical_and(r >= 1, z - r >= 0))
        def _():
            move(KV_UP, z - r, y, c, up).wait_recv()
            spread_kv(z - r)

        @pl.when(jnp.logical_and(r >= 1, z - r >= 0))
        def _():
            move(W_UP, z - r, y, c, up, mine).wait_recv()
            pl.when(has_up)(lambda: move(W_UP, z - r, y, c, up, mine).start())
            move(W_Y, z - r, y, c, other_y, mine).start()
            onward(z - r, y)

        @pl.when(jnp.logical_and(r >= 1, z + r < planes))
        def _():
            move(W_DOWN, z + r, y, c, down, mine).wait_recv()
            pl.when(has_down)(lambda: move(W_DOWN, z + r, y, c, down, mine).start())
            move(W_Y, z + r, y, c, other_y, mine).start()
            onward(z + r, y)

        def from_y(zp):
            move(W_Y, zp, 1 - y, c, other_y, mine).wait_recv()
            onward(zp, 1 - y)

        each_plane(r - 1, from_y)

        @pl.when(jnp.logical_and(r >= 1, z - r + 1 >= 0))
        def _():
            move(KV_Y, z - r + 1, 1 - y, c, other_y).wait_recv()
            move(KV_CORE, z - r + 1, 1 - y, c, other_core).start()

        def from_x(zp):
            def one(yp):
                move(W_X, zp, yp, c, over_x, taken).wait_recv()
                move(W_CORE_X, zp, yp, c, other_core, taken).start()

            pl.when(zp != z)(lambda: one(y))
            one(1 - y)

        each_plane(r - 2, from_x)
        pl.when(jnp.logical_and(r >= 1, z - r + 1 >= 0))(lambda: attend(z - r + 1))

        @pl.when(r == planes)
        def _():
            finish_attention()

            def near_plane(d, carry):
                each_plane(d, project)
                return carry

            lax.fori_loop(0, planes - 1, near_plane, 0)

        return carry

    lax.fori_loop(0, planes + 2, weight_round, 0)
    each_plane(planes - 1, project)

    def finish_tile(t, carry):
        squares, dots = carry
        cols = pl.ds(pl.multiple_of(t * tile, tile), tile)
        stream = projected[:, cols].astype(jnp.bfloat16)
        stream_ref[:, cols] = stream
        widened = stream.astype(jnp.float32)
        squares += jnp.sum(widened * widened, axis=1, keepdims=True)
        dots += jnp.sum(widened * gain_ref[:, cols], axis=1, keepdims=True)
        return squares, dots

    zero = jnp.zeros((tok, 1), jnp.float32)
    squares, dots = lax.fori_loop(0, width // tile, finish_tile, (zero, zero))
    scored = dots * lax.rsqrt(squares / width + 1e-06)
    values_ref[...] = jnp.where(row_ok, scored, 0.0)

    def drain(zp, carry):
        @pl.when(zp <= z)
        def _():
            pl.when(has_up)(lambda: move(KV_UP, zp, y, c, up).wait_send())
            pl.when(has_up)(lambda: move(W_UP, zp, y, c, up, mine).wait_send())
            move(KV_Y, zp, y, c, other_y).wait_send()
            move(KV_CORE, zp, y, c, other_core).wait_send()
            move(KV_CORE, zp, 1 - y, c, other_core).wait_send()

        @pl.when(jnp.logical_and(zp >= z, has_down))
        def _():
            move(W_DOWN, zp, y, c, down, mine).wait_send()

        move(W_Y, zp, y, c, other_y, mine).wait_send()

        def sent(yp):
            move(W_X, zp, yp, c, over_x, given).wait_send()
            move(W_CORE, zp, yp, c, other_core, mine).wait_send()
            move(W_CORE_X, zp, yp, c, other_core, taken).wait_send()

        sent(1 - y)
        pl.when(zp != z)(lambda: sent(y))
        pl.when(zp == z)(lambda: move(W_CORE, zp, y, c, other_core, whole).wait_send())
        return carry

    lax.fori_loop(0, planes, drain, 0)


def per_device(
    devices,
    queries,
    key_rows,
    value_rows,
    residual,
    out_weight,
    norm_gain,
    value_head,
    valid_length,
):
    tok, q_width = queries.shape
    width = residual.shape[1]
    heads = q_width // HEAD_DIM
    planes = devices // PLANE
    any_space = pl.BlockSpec(memory_space=pl.ANY)
    vmem = pl.BlockSpec(memory_space=pltpu.VMEM)
    stream, scored = pl.pallas_call(
        functools.partial(kernel, planes),
        name="critic_block",
        out_shape=(
            jax.ShapeDtypeStruct((tok, width), jnp.bfloat16),
            jax.ShapeDtypeStruct((tok, 1), jnp.float32),
        ),
        in_specs=[pl.BlockSpec(memory_space=pltpu.SMEM)] + [any_space] * 5 + [vmem],
        out_specs=(vmem, vmem),
        scratch_shapes=[
            pltpu.VMEM((tok, q_width), jnp.bfloat16),
            pltpu.VMEM((devices, tok, 2 * key_rows.shape[1]), jnp.bfloat16),
            pltpu.VMEM((devices,) + out_weight.shape, jnp.bfloat16),
            pltpu.VMEM((tok, width), jnp.bfloat16),
            pltpu.VMEM((planes, tok, q_width // planes), jnp.bfloat16),
            pltpu.VMEM((tok, width), jnp.float32),
            pltpu.VMEM((heads, tok, 1), jnp.float32),
            pltpu.VMEM((heads, tok, 1), jnp.float32),
            pltpu.VMEM((heads, tok, HEAD_DIM), jnp.float32),
            pltpu.SemaphoreType.DMA((9, ROWS_Y * planes)),
            pltpu.SemaphoreType.DMA((9, ROWS_Y * planes)),
            pltpu.SemaphoreType.DMA((5,)),
        ],
        compiler_params=pltpu.CompilerParams(
            collective_id=0, has_side_effects=True, vmem_limit_bytes=60 * 1024 * 1024
        ),
    )(
        valid_length,
        queries,
        key_rows,
        value_rows,
        residual,
        out_weight,
        (norm_gain * value_head)[None, :],
    )
    return stream, scored[:, 0]


def solution(mesh):
    rows = P(("league", "seq"), None)
    return jax.shard_map(
        functools.partial(per_device, mesh.shape["seq"]),
        mesh=mesh,
        in_specs=(rows, rows, rows, rows, P("seq", None), P(), P(), P("league")),
        out_specs=(rows, P(("league", "seq"))),
        check_vma=False,
    )
```
